32 devices in a mesh: dp: 1 (over z), tp: 32 (over y, x, core).
Axes of the slice: x: 4, y: 4, z: 1, core: 2. Of those that a mesh axis runs over, the one named last changes fastest.
The devices are a block of a 4x4x8 slice.
Arguments:
- hid_one: bfloat16 [256, 9, 2048], P('dp')
- q_one: float32 [256, 8, 32000], P(('dp', 'tp'))
- tok_one: int32 [256, 8], P('dp')
- hid_two: bfloat16 [256, 9, 2048], P('dp')
- q_two: float32 [256, 8, 32000], P(('dp', 'tp'))
- tok_two: int32 [256, 8], P('dp')
- w_head: bfloat16 [2048, 32000], P(None, 'tp')
Outputs:
- output 1: float32 [256, 8], P('dp')
- output 2: float32 [256], P('dp')
- output 3: float32 [256, 8, 32000], P('dp', None, 'tp')
- output 4: float32 [256, 32000], P('dp', 'tp')
- output 5: float32 [256, 8], P('dp')
- output 6: float32 [256], P('dp')
- output 7: float32 [256, 8, 32000], P('dp', None, 'tp')
- output 8: float32 [256, 32000], P('dp', 'tp')
All inputs are finite; a program needn't handle non-finite values.
Results may differ from the reference program's by a relative error of at most 0.001.
Values are sent between devices in bfloat16 or wider.
A program may use at most 768 MiB of HBM per device.

```python
import jax
import jax.numpy as jnp
from jax import lax

BATCH_ROWS = 256
DRAFT_LEN = 8
HIDDEN = 2048
VOCAB_SIZE = 32000
BLOCK_ROWS = 4
INV_TEMP = 1.25


def draw_microbatch(key_hid, key_q, key_tok):
    hidden = jax.random.normal(key_hid, (BATCH_ROWS, DRAFT_LEN + 1, HIDDEN), jnp.float32)
    q_logit = jax.random.normal(key_q, (BATCH_ROWS, DRAFT_LEN, VOCAB_SIZE), jnp.float32)
    q_prob = jax.nn.softmax(q_logit, axis=-1)
    tokens = jax.random.randint(key_tok, (BATCH_ROWS, DRAFT_LEN), 0, VOCAB_SIZE, jnp.int32)
    return hidden.astype(jnp.bfloat16), q_prob, tokens


def setup_inputs(seed: int = 0, part: int = 0) -> dict:
    base_key = jax.random.key(seed)
    shared_key, parts_key = jax.random.split(base_key)
    part_key = jax.random.fold_in(parts_key, part)
    key_list = jax.random.split(part_key, 6)
    w_head = jax.random.normal(shared_key, (HIDDEN, VOCAB_SIZE), jnp.float32) * HIDDEN ** -0.5
    hid_one, q_one, tok_one = draw_microbatch(key_list[0], key_list[1], key_list[2])
    hid_two, q_two, tok_two = draw_microbatch(key_list[3], key_list[4], key_list[5])
    return {'hid_one': hid_one, 'q_one': q_one, 'tok_one': tok_one, 'hid_two': hid_two, 'q_two': q_two, 'tok_two': tok_two, 'w_head': w_head.astype(jnp.bfloat16)}


def verify_block(hid_blk, q_blk, tok_blk, w_head):
    n_rows = hid_blk.shape[0]
    flat_rows = hid_blk.reshape(n_rows * (DRAFT_LEN + 1), HIDDEN)
    logits = jnp.dot(flat_rows, w_head, preferred_element_type=jnp.float32) * INV_TEMP
    logits = logits.reshape(n_rows, DRAFT_LEN + 1, VOCAB_SIZE)
    row_max = jnp.max(logits, axis=-1, keepdims=True)
    exp_val = jnp.exp(logits - row_max)
    prob_all = exp_val / jnp.sum(exp_val, axis=-1, keepdims=True)
    p_draft = prob_all[:, :DRAFT_LEN]
    p_pick = jnp.take_along_axis(p_draft, tok_blk[:, :, None], axis=-1)[:, :, 0]
    q_pick = jnp.take_along_axis(q_blk, tok_blk[:, :, None], axis=-1)[:, :, 0]
    accept = jnp.minimum(p_pick / q_pick, 1.0)
    excess = jnp.maximum(p_draft - q_blk, 0.0)
    residual = excess / jnp.sum(excess, axis=-1, keepdims=True)
    return accept, residual, prob_all[:, DRAFT_LEN]


def verify_batch(hidden, q_prob, tokens, w_head):
    n_blocks = BATCH_ROWS // BLOCK_ROWS
    blocks = (hidden.reshape(n_blocks, BLOCK_ROWS, DRAFT_LEN + 1, HIDDEN), q_prob.reshape(n_blocks, BLOCK_ROWS, DRAFT_LEN, VOCAB_SIZE), tokens.reshape(n_blocks, BLOCK_ROWS, DRAFT_LEN))
    accept, residual, bonus_prob = lax.map(lambda block_in: verify_block(block_in[0], block_in[1], block_in[2], w_head), blocks)
    accept = accept.reshape(BATCH_ROWS, DRAFT_LEN)
    expect = jnp.sum(jnp.cumprod(accept, axis=1), axis=1)
    return accept, expect, residual.reshape(BATCH_ROWS, DRAFT_LEN, VOCAB_SIZE), bonus_prob.reshape(BATCH_ROWS, VOCAB_SIZE)


def reference(hid_one, q_one, tok_one, hid_two, q_two, tok_two, w_head):
    out_one = verify_batch(hid_one, q_one, tok_one, w_head)
    out_two = verify_batch(hid_two, q_two, tok_two, w_head)
    return (out_one[0], out_one[1], out_one[2], out_one[3], out_two[0], out_two[1], out_two[2], out_two[3])
```

```python
import functools
import math

import jax
import jax.numpy as jnp
from jax import lax
from jax.experimental import pallas as pl
from jax.experimental.pallas import tpu as pltpu
from jax.sharding import PartitionSpec as P

INV_TEMP = 1.25
LANES = 128
SUBLANES = 8
SLOTS = 8
HEAD_ROUNDS = 4
COL_TILE = 256
MESH = pl.DeviceIdType.MESH


def partner_steps(n):
    side = math.isqrt(n // 2)
    groups = {}
    for dy in range(side):
        for dx in range(side):
            hops = tuple(sorted((min(dy, side - dy), min(dx, side - dx)), reverse=True))
            groups.setdefault(hops, []).append((dy, dx))
    order = [(2, 2), (2, 1), (2, 0), (1, 0), (1, 1), (0, 0)]
    order += [k for k in groups if k not in order]
    steps = []
    for key in order:
        for dc in range(2):
            for dy, dx in groups.get(key, []):
                if (dy, dx, dc) != (0, 0, 0):
                    steps.append((dy, dx, dc))
    return steps


def exchange_kernel(n, hid_one, hid_two, q_one, q_two, tok_one, tok_two, w_hbm,
                    ex, eb, fin,
                    w_buf, hid_buf, q_buf, stage, recv, loc_max, tok_buf,
                    st_send, st_recv, st_out, st_res, z_send, z_recv, z_out, z_res,
                    q_sem, w_sem, hid_sem, send_sem, recv_sem, st_sem, z_sem):
    me = lax.axis_index('tp')
    depth, batch = tok_one.shape
    vocab = w_hbm.shape[0]
    halves = batch // LANES
    rounds = 2 * depth
    hids, qs, toks = (hid_one, hid_two), (q_one, q_two), (tok_one, tok_two)
    side = math.isqrt(n // 2)
    core, chip = lax.rem(me, 2), me // 2
    col, row = lax.rem(chip, side), chip // side
    steps = partner_steps(n)

    def partner(step):
        dy, dx, dc = step
        return (lax.rem(row + dy, side) * side + lax.rem(col + dx, side)) * 2 + lax.rem(core + dc, 2)

    barrier = pltpu.get_barrier_semaphore()
    for step in steps:
        pl.semaphore_signal(barrier, inc=1, device_id={'tp': partner(step)}, device_id_type=MESH)

    q_tiles = q_one.shape[1] // LANES

    def load_q(mb):
        def one(t, carry):
            cols = pl.ds(pl.multiple_of(t * LANES, LANES), LANES)
            pltpu.make_async_copy(qs[mb].at[:, cols], q_buf.at[t], q_sem).start()
            return carry

        lax.fori_loop(0, q_tiles, one, 0)

    def wait_q():
        block = q_buf.at[pl.ds(0, q_tiles)]
        pltpu.make_async_copy(block, block, q_sem).wait()

    def load_hid(mb, i, slot):
        return pltpu.make_async_copy(hids[mb].at[i], hid_buf.at[slot], hid_sem.at[slot])

    load_q(0)
    load_w = pltpu.make_async_copy(w_hbm, w_buf, w_sem)
    load_w.start()
    load_hid(0, 0, 0).start()
    st_send[...] = jnp.zeros_like(st_send)
    z_send[...] = jnp.zeros_like(z_send)
    st_out[...] = jnp.zeros_like(st_out)
    z_out[...] = jnp.zeros_like(z_out)
    for g in range(rounds):
        i = g % depth
        tok_buf[g] = toks[g // depth][i:i + 1, :]
    lane = lax.broadcasted_iota(jnp.int32, (SUBLANES, LANES), 1)
    tiles = pl.cdiv(vocab, LANES)

    def pack(r):
        i, slot = lax.rem(r, depth), lax.rem(r, SLOTS)

        def one(d, carry):
            start = d * vocab
            base, off = start // LANES, lax.rem(start, LANES)
            shift = lax.rem(LANES - off, LANES)
            rolled = []
            for t in range(tiles + 1):
                rolled.append(pltpu.roll(q_buf[base + t, pl.ds(i, SUBLANES, stride=depth), :], shift, 1))
            for t in range(tiles):
                stage[slot, d, :, t * LANES:(t + 1) * LANES] = jnp.where(lane < LANES - off, rolled[t], rolled[t + 1])
            return carry

        lax.fori_loop(0, n, one, 0)

    def send(r):
        slot = lax.rem(r, SLOTS)
        mine = pl.ds(pl.multiple_of(me * SUBLANES, SUBLANES), SUBLANES)
        for step in steps:
            to = partner(step)
            pltpu.make_async_remote_copy(
                src_ref=stage.at[slot, to], dst_ref=recv.at[r, mine],
                send_sem=send_sem.at[slot], recv_sem=recv_sem.at[r],
                device_id={'tp': to}, device_id_type=MESH).start()
        recv[r, mine, :] = stage[slot, me]

    def wait_send(r):
        block = stage.at[lax.rem(r, SLOTS), pl.ds(0, n - 1)]
        pltpu.make_async_copy(block, block, send_sem.at[lax.rem(r, SLOTS)]).wait()

    def wait_tiles(ref, sem):
        block = ref.at[pl.ds(0, n - 1)]
        pltpu.make_async_copy(block, block, sem).wait()

    wait_q()
    pack(0)
    pl.semaphore_wait(barrier, n - 1)
    send(0)

    def head_round(r, carry):
        pack(r)
        send(r)
        return carry

    lax.fori_loop(1, HEAD_ROUNDS, head_round, 0)

    load_w.wait()
    spans = [(v, min(COL_TILE, vocab - v)) for v in range(0, vocab, COL_TILE)]

    def logits(hid_slot, out):
        top = None
        for v, size in spans:
            z = lax.dot_general(w_buf[v:v + size, :], hid_buf[hid_slot], (((1,), (1,)), ((), ())),
                                preferred_element_type=jnp.float32) * INV_TEMP
            out[v:v + size, :] = z
            m = jnp.max(z, axis=0, keepdims=True)
            top = m if top is None else jnp.maximum(top, m)
        total = jnp.zeros_like(top)
        for v, size in spans:
            e = jnp.exp(out[v:v + size, :] - top)
            out[v:v + size, :] = e
            total = total + jnp.sum(e, axis=0, keepdims=True)
        return top, total

    for mb in range(2):
        first = mb * (depth + 1)

        def position(i, carry, mb=mb, first=first):
            slot = lax.rem(first + i, 2)
            load_hid(mb, i + 1, 1 - slot).start()
            load_hid(mb, i, slot).wait()
            g = mb * depth + i
            top, total = logits(slot, ex.at[g])
            loc_max[g] = top
            for h in range(halves):
                st_send[g * halves + h, 0:1, :] = top[:, h * LANES:(h + 1) * LANES]
                st_send[g * halves + h, 1:2, :] = total[:, h * LANES:(h + 1) * LANES]
            return carry

        lax.fori_loop(0, depth, position, 0)
        slot = (first + depth) % 2
        if mb == 0:
            load_hid(1, 0, 1 - slot).start()
        load_hid(mb, depth, slot).wait()
        top, total = logits(slot, eb.at[mb])
        loc_max[rounds + mb] = top
        for i in range(depth):
            for h in range(halves):
                d = (mb * depth + i) * halves + h
                st_send[d, 2:3, :] = top[:, h * LANES:(h + 1) * LANES]
                st_send[d, 3:4, :] = total[:, h * LANES:(h + 1) * LANES]

    def scatter(src, dst, sems):
        for step in steps:
            to = partner(step)
            pltpu.make_async_remote_copy(
                src_ref=src.at[to], dst_ref=dst.at[me], send_sem=sems.at[0], recv_sem=sems.at[1],
                device_id={'tp': to}, device_id_type=MESH).start()
        dst[me] = src[me]

    def spread(src, dst, sems):
        for step in steps:
            pltpu.make_async_remote_copy(
                src_ref=src, dst_ref=dst.at[me], send_sem=sems.at[2], recv_sem=sems.at[3],
                device_id={'tp': partner(step)}, device_id_type=MESH).start()
        dst[me] = src[...]

    scatter(st_send, st_recv, st_sem)
    lax.fori_loop(HEAD_ROUNDS, HEAD_ROUNDS + 2, head_round, 0)
    wait_tiles(st_recv, st_sem.at[1])
    for r in (0, 2):
        m = st_recv[:, r, :]
        top = jnp.max(m, axis=0, keepdims=True)
        total = jnp.sum(st_recv[:, r + 1, :] * jnp.exp(m - top), axis=0, keepdims=True)
        st_out[r:r + 1, :] = top
        st_out[r + 1:r + 2, :] = 1.0 / total
    spread(st_out, st_res, st_sem)
    lax.fori_loop(HEAD_ROUNDS + 2, depth, head_round, 0)
    load_q(1)
    wait_tiles(st_res, st_sem.at[3])

    for mb in range(2):
        for h in range(halves):
            d = mb * depth * halves + h
            lanes = slice(h * LANES, (h + 1) * LANES)
            f = jnp.exp(loc_max[rounds + mb][:, lanes] - st_res[d, 2:3, :]) * st_res[d, 3:4, :]
            eb[mb, :, lanes] = eb[mb, :, lanes] * f

    def process(g):
        block = recv.at[g, pl.ds(0, (n - 1) * SUBLANES)]
        pltpu.make_async_copy(block, block, recv_sem.at[g]).wait()
        for h in range(halves):
            lanes = slice(h * LANES, (h + 1) * LANES)
            d = g * halves + h
            f = jnp.exp(loc_max[g][:, lanes] - st_res[d, 0:1, :]) * st_res[d, 1:2, :]
            tok = tok_buf[g][:, lanes] - me * vocab

            def tile(v, size, sums):
                qt = recv[g, lanes, pl.ds(v, LANES)].T[:size]
                p = ex[g, pl.ds(v, size), lanes] * f
                x = jnp.maximum(p - qt, 0.0)
                ex[g, pl.ds(v, size), lanes] = x
                hit = lax.broadcasted_iota(jnp.int32, (size, LANES), 0) == tok - v
                zero = jnp.zeros_like(qt)
                parts = (x, jnp.where(hit, qt, zero), jnp.where(hit, p, zero))
                return tuple(s + jnp.sum(a, axis=0, keepdims=True) for s, a in zip(sums, parts))

            zero = jnp.zeros((1, LANES), jnp.float32)
            whole = vocab // LANES
            sums = lax.fori_loop(
                0, whole, lambda t, s: tile(pl.multiple_of(t * LANES, LANES), LANES, s), (zero, zero, zero))
            if vocab % LANES:
                sums = tile(whole * LANES, vocab % LANES, sums)
            for k in range(3):
                z_send[d, k:k + 1, :] = sums[k]

            @pl.when(me != d)
            def _():
                pltpu.make_async_remote_copy(
                    src_ref=z_send.at[d], dst_ref=z_recv.at[me], send_sem=z_sem.at[0], recv_sem=z_sem.at[1],
                    device_id={'tp': d}, device_id_type=MESH).start()

            @pl.when(me == d)
            def _():
                z_recv[me] = z_send[d]

    wait_q()

    def main_round(r, carry):
        wait_send(r - SLOTS)
        pack(r)
        send(r)
        process(r - SLOTS)
        return carry

    lax.fori_loop(depth, rounds, main_round, 0)

    def tail_round(g, carry):
        process(g)
        return carry

    lax.fori_loop(rounds - SLOTS, rounds, tail_round, 0)

    wait_tiles(z_recv, z_sem.at[1])
    sums = jnp.sum(z_recv[...], axis=0)
    z_out[0:1, :] = 1.0 / sums[0:1]
    z_out[1:2, :] = jnp.minimum(sums[2:3] / sums[1:2], 1.0)
    spread(z_out, z_res, z_sem)

    def drain(r, carry):
        wait_send(r)
        return carry

    lax.fori_loop(rounds - SLOTS, rounds, drain, 0)
    wait_tiles(st_send, st_sem.at[0])
    wait_tiles(st_res, st_sem.at[2])
    wait_tiles(z_send, z_sem.at[0])
    wait_tiles(z_res, z_sem.at[3])
    fin[...] = z_res[...]
    wait_tiles(z_res, z_sem.at[2])


def finish_kernel(depth, ex, eb, fin, res_one, res_two, bon_one, bon_two, acc_one, acc_two, exp_one, exp_two,
                  buf, sem, b_sem):
    ress, bons, accs, exps = (res_one, res_two), (bon_one, bon_two), (acc_one, acc_two), (exp_one, exp_two)
    halves = eb.shape[2] // LANES
    slots = buf.shape[0]
    for mb in range(2):
        pltpu.make_async_copy(eb.at[mb], bons[mb], b_sem.at[mb]).start()
    pending = []
    for mb in range(2):
        for i in range(depth):
            g = mb * depth + i
            if g >= slots:
                pending[g - slots].wait()
            for h in range(halves):
                lanes = slice(h * LANES, (h + 1) * LANES)
                buf[g % slots, :, lanes] = ex[g, :, lanes] * fin[g * halves + h, 0:1, :]
            copy = pltpu.make_async_copy(buf.at[g % slots], ress[mb].at[i], sem.at[g % slots])
            copy.start()
            pending.append(copy)
    for mb in range(2):
        for h in range(halves):
            lanes = slice(h * LANES, (h + 1) * LANES)
            prod = jnp.ones((1, LANES), jnp.float32)
            total = jnp.zeros((1, LANES), jnp.float32)
            for i in range(depth):
                a = fin[(mb * depth + i) * halves + h, 1:2, :]
                accs[mb][i:i + 1, lanes] = a
                prod = prod * a
                total = total + prod
            exps[mb][:, lanes] = total
    for copy in pending[-slots:]:
        copy.wait()
    for mb in range(2):
        pltpu.make_async_copy(eb.at[mb], bons[mb], b_sem.at[mb]).wait()


def verify_both(n, hid_one, q_one, tok_one, hid_two, q_two, tok_two, w_local):
    seqs, depth, whole_vocab = q_one.shape
    batch, vocab, hidden = hid_one.shape[0], w_local.shape[1], hid_one.shape[2]
    halves = batch // LANES
    rounds = 2 * depth
    width = pl.cdiv(vocab, LANES) * LANES
    assert seqs == SUBLANES and rounds * halves == n and batch == n * seqs
    f32 = jnp.float32
    vmem = pl.BlockSpec(memory_space=pltpu.VMEM)
    anys = pl.BlockSpec(memory_space=pl.ANY)
    tile = (n, SUBLANES, LANES)
    ex, eb, fin = pl.pallas_call(
        functools.partial(exchange_kernel, n),
        out_shape=(pltpu.VMEM((rounds, vocab, batch), f32), pltpu.VMEM((2, vocab, batch), f32), pltpu.VMEM(tile, f32)),
        in_specs=[anys, anys, anys, anys, vmem, vmem, anys],
        out_specs=(vmem, vmem, vmem),
        scratch_shapes=[
            pltpu.VMEM((vocab, hidden), w_local.dtype),
            pltpu.VMEM((2, batch, hidden), hid_one.dtype),
            pltpu.VMEM((whole_vocab // LANES + 1, seqs * depth, LANES), f32),
            pltpu.VMEM((SLOTS, n, SUBLANES, width), f32),
            pltpu.VMEM((rounds, batch, width), f32),
            pltpu.VMEM((rounds + 2, 1, batch), f32),
            pltpu.VMEM((rounds, 1, batch), jnp.int32),
            pltpu.VMEM(tile, f32), pltpu.VMEM(tile, f32), pltpu.VMEM(tile[1:], f32), pltpu.VMEM(tile, f32),
            pltpu.VMEM(tile, f32), pltpu.VMEM(tile, f32), pltpu.VMEM(tile[1:], f32), pltpu.VMEM(tile, f32),
            pltpu.SemaphoreType.DMA, pltpu.SemaphoreType.DMA, pltpu.SemaphoreType.DMA((2,)),
            pltpu.SemaphoreType.DMA((SLOTS,)), pltpu.SemaphoreType.DMA((rounds,)),
            pltpu.SemaphoreType.DMA((4,)), pltpu.SemaphoreType.DMA((4,)),
        ],
        compiler_params=pltpu.CompilerParams(collective_id=0, has_side_effects=True, vmem_limit_bytes=44 * 2 ** 20),
        name='exchange',
    )(jnp.swapaxes(hid_one, 0, 1), jnp.swapaxes(hid_two, 0, 1),
      q_one.reshape(seqs * depth, whole_vocab), q_two.reshape(seqs * depth, whole_vocab),
      tok_one.T, tok_two.T, w_local.T)

    shapes = [(depth, vocab, batch)] * 2 + [(vocab, batch)] * 2 + [(depth, batch)] * 2 + [(1, batch)] * 2
    outs = pl.pallas_call(
        functools.partial(finish_kernel, depth),
        out_shape=[jax.ShapeDtypeStruct(s, f32) for s in shapes],
        in_specs=[vmem] * 3,
        out_specs=[anys] * 4 + [vmem] * 4,
        scratch_shapes=[pltpu.VMEM((4, vocab, batch), f32), pltpu.SemaphoreType.DMA((4,)), pltpu.SemaphoreType.DMA((2,))],
        compiler_params=pltpu.CompilerParams(vmem_limit_bytes=12 * 2 ** 20),
        name='finish',
    )(ex, eb, fin)
    res, bon, acc, tot = outs[0:2], outs[2:4], outs[4:6], outs[6:8]
    result = ()
    for mb in range(2):
        result += (acc[mb].T, tot[mb].reshape(batch), jnp.transpose(res[mb], (2, 0, 1)), bon[mb].T)
    return result


def solution(mesh):
    row_spec = P('dp')
    q_spec = P(('dp', 'tp'))
    w_spec = P(None, 'tp')
    vocab_spec = P('dp', None, 'tp')
    bonus_spec = P('dp', 'tp')
    out_specs = (row_spec, row_spec, vocab_spec, bonus_spec) * 2
    in_specs = (row_spec, q_spec, row_spec, row_spec, q_spec, row_spec, w_spec)
    return jax.shard_map(functools.partial(verify_both, mesh.shape['tp']), mesh=mesh,
                         in_specs=in_specs, out_specs=out_specs, check_vma=False)
```

```python
import functools
import math

import jax
import jax.numpy as jnp
from jax import lax
from jax.experimental import pallas as pl
from jax.experimental.pallas import tpu as pltpu
from jax.sharding import PartitionSpec as P

INV_TEMP = 1.25
LANES = 128
SUBLANES = 8
SLOTS = 8
HEAD_ROUNDS = 4
COL_TILE = 256
LATE_ROUNDS = 2
UNROLL = 7
PACK_UNROLL = 4
MESH = pl.DeviceIdType.MESH


def partner_steps(side):
    one, back, half = 1, side - 1, side // 2
    classes = [
        [(half, one), (half, back), (one, half), (back, half)],
        [(half, half)],
        [(half, 0), (0, half)],
        [(one, one), (back, back)],
        [(one, back), (back, one)],
        [(one, 0), (back, 0), (0, one), (0, back)],
        [(0, 0)],
    ]
    assert sorted(d for c in classes for d in c) == [(x, y) for x in range(side) for y in range(side)]
    return [(dx, dy, dc) for c in classes for dc in range(2) for dx, dy in c if (dx, dy, dc) != (0, 0, 0)]


def exchange_kernel(n, hid_one, hid_two, q_one, q_two, tok_one, tok_two, w_hbm,
                    ex, eb, fin,
                    w_buf, hid_buf, q_buf, stage, recv, loc_max, tok_buf,
                    st_send, st_recv, st_out, st_res, z_send, z_recv, z_out, z_res, late_send, late_recv, guests,
                    q_sem, w_sem, hid_sem, send_sem, recv_sem, st_sem, z_sem, late_sem):
    me = lax.axis_index('tp')
    depth, batch = tok_one.shape
    vocab = w_hbm.shape[0]
    halves = batch // LANES
    rounds = 2 * depth
    early = (rounds - LATE_ROUNDS) * halves
    hids, qs, toks = (hid_one, hid_two), (q_one, q_two), (tok_one, tok_two)
    side = math.isqrt(n // 2)
    core, chip = lax.rem(me, 2), me // 2
    col, row = lax.rem(chip, side), chip // side
    steps = partner_steps(side)

    def partner(step):
        dx, dy, dc = step
        dy = dy + core * ((side - dy) % side - dy)
        return (lax.rem(row + dy, side) * side + lax.rem(col + dx, side)) * 2 + lax.rem(core + dc, 2)

    barrier = pltpu.get_barrier_semaphore()
    for step in steps:
        pl.semaphore_signal(barrier, inc=1, device_id={'tp': partner(step)}, device_id_type=MESH)

    q_tiles = q_one.shape[1] // LANES

    def load_q(mb):
        def one(t, carry):
            cols = pl.ds(pl.multiple_of(t * LANES, LANES), LANES)
            pltpu.make_async_copy(qs[mb].at[:, cols], q_buf.at[t], q_sem).start()
            return carry

        lax.fori_loop(0, q_tiles, one, 0)

    def wait_q():
        block = q_buf.at[pl.ds(0, q_tiles)]
        pltpu.make_async_copy(block, block, q_sem).wait()

    def load_hid(mb, i, slot):
        return pltpu.make_async_copy(hids[mb].at[i], hid_buf.at[slot], hid_sem.at[slot])

    load_q(0)
    load_w = pltpu.make_async_copy(w_hbm, w_buf, w_sem)
    load_w.start()
    load_hid(0, 0, 0).start()
    for g in range(rounds):
        i = g % depth
        tok_buf[g] = toks[g // depth][i:i + 1, :]
    lane = lax.broadcasted_iota(jnp.int32, (SUBLANES, LANES), 1)
    tiles = pl.cdiv(vocab, LANES)
    used = vocab - (tiles - 1) * LANES
    gap = LANES - used
    spread_pos = pl.cdiv(used, gap)
    assert spread_pos < depth and gap % SUBLANES == 0

    def narrow(r, action):
        @pl.when(lax.rem(r, depth) == spread_pos)
        def _():
            action((tiles - 1) * LANES)

        @pl.when(lax.rem(r, depth) != spread_pos)
        def _():
            action(tiles * LANES)

    def pack(r):
        i, slot = lax.rem(r, depth), lax.rem(r, SLOTS)
        to_gap = lax.rem(used + depth * LANES - gap * i, LANES)

        def one(d, carry):
            start = d * vocab
            base, off = start // LANES, lax.rem(start, LANES)
            shift = lax.rem(LANES - off, LANES)
            rolled = []
            for t in range(tiles + 1):
                rolled.append(pltpu.roll(q_buf[base + t, pl.ds(i, SUBLANES, stride=depth), :], shift, 1))
            for t in range(tiles - 1):
                stage[slot, d, :, t * LANES:(t + 1) * LANES] = jnp.where(lane < LANES - off, rolled[t], rolled[t + 1])
            last = jnp.where(lane < LANES - off, rolled[tiles - 1], rolled[tiles])
            guest = [pltpu.roll(q_buf[base + t, pl.ds(spread_pos, SUBLANES, stride=depth), :], shift, 1)
                     for t in (tiles - 1, tiles)]
            guest = pltpu.roll(jnp.where(lane < LANES - off, guest[0], guest[1]), to_gap, 1)
            stage[slot, d, :, (tiles - 1) * LANES:] = jnp.where(lane < used, last, guest)
            return carry

        lax.fori_loop(0, n, one, 0, unroll=PACK_UNROLL)

    def send(r):
        slot = lax.rem(r, SLOTS)
        mine = pl.ds(pl.multiple_of(me * SUBLANES, SUBLANES), SUBLANES)

        def start(width):
            for step in steps:
                to = partner(step)
                pltpu.make_async_remote_copy(
                    src_ref=stage.at[slot, to, :, pl.ds(0, width)], dst_ref=recv.at[r, mine, pl.ds(0, width)],
                    send_sem=send_sem.at[slot], recv_sem=recv_sem.at[r],
                    device_id={'tp': to}, device_id_type=MESH).start()

        narrow(r, start)
        recv[r, mine, :] = stage[slot, me]

    def wait_send(r):
        def wait(width):
            block = stage.at[lax.rem(r, SLOTS), pl.ds(0, n - 1), :, pl.ds(0, width)]
            pltpu.make_async_copy(block, block, send_sem.at[lax.rem(r, SLOTS)]).wait()

        narrow(r, wait)

    def wait_tiles(ref, sem):
        block = ref.at[pl.ds(0, n - 1)]
        pltpu.make_async_copy(block, block, sem).wait()

    wait_q()
    pack(0)
    pl.semaphore_wait(barrier, n - 1)
    send(0)

    def head_round(r, carry):
        pack(r)
        send(r)
        return carry

    lax.fori_loop(1, HEAD_ROUNDS, head_round, 0)

    load_w.wait()
    spans = [(v, min(COL_TILE, vocab - v)) for v in range(0, vocab, COL_TILE)]

    def logits(hid_slot, out):
        top = None
        for v, size in spans:
            z = lax.dot_general(w_buf[v:v + size, :], hid_buf[hid_slot], (((1,), (1,)), ((), ())),
                                preferred_element_type=jnp.float32) * INV_TEMP
            out[v:v + size, :] = z
            m = jnp.max(z, axis=0, keepdims=True)
            top = m if top is None else jnp.maximum(top, m)
        total = jnp.zeros_like(top)
        for v, size in spans:
            e = jnp.exp(out[v:v + size, :] - top)
            out[v:v + size, :] = e
            total = total + jnp.sum(e, axis=0, keepdims=True)
        return top, total

    for mb in range(2):
        first = mb * (depth + 1)

        def position(i, carry, mb=mb, first=first):
            slot = lax.rem(first + i, 2)
            load_hid(mb, i + 1, 1 - slot).start()
            load_hid(mb, i, slot).wait()
            g = mb * depth + i
            top, total = logits(slot, ex.at[g])
            loc_max[g] = top
            for h in range(halves):
                st_send[g * halves + h, 0:1, :] = top[:, h * LANES:(h + 1) * LANES]
                st_send[g * halves + h, 1:2, :] = total[:, h * LANES:(h + 1) * LANES]
            return carry

        lax.fori_loop(0, depth, position, 0)
        slot = (first + depth) % 2
        if mb == 0:
            load_hid(1, 0, 1 - slot).start()
        load_hid(mb, depth, slot).wait()
        top, total = logits(slot, eb.at[mb])
        loc_max[rounds + mb] = top
        for i in range(depth):
            for h in range(halves):
                d = (mb * depth + i) * halves + h
                st_send[d, 2:3, :] = top[:, h * LANES:(h + 1) * LANES]
                st_send[d, 3:4, :] = total[:, h * LANES:(h + 1) * LANES]

    def scatter(src, dst, sems):
        for step in steps:
            to = partner(step)
            pltpu.make_async_remote_copy(
                src_ref=src.at[to], dst_ref=dst.at[me], send_sem=sems.at[0], recv_sem=sems.at[1],
                device_id={'tp': to}, device_id_type=MESH).start()
        dst[me] = src[me]

    def spread(src, dst, sems):
        for step in steps:
            pltpu.make_async_remote_copy(
                src_ref=src, dst_ref=dst.at[me], send_sem=sems.at[2], recv_sem=sems.at[3],
                device_id={'tp': partner(step)}, device_id_type=MESH).start()
        dst[me] = src[...]

    scatter(st_send, st_recv, st_sem)
    lax.fori_loop(HEAD_ROUNDS, HEAD_ROUNDS + 2, head_round, 0)
    wait_tiles(st_recv, st_sem.at[1])
    for r in (0, 2):
        m = st_recv[:, r, :]
        top = jnp.max(m, axis=0, keepdims=True)
        total = jnp.sum(st_recv[:, r + 1, :] * jnp.exp(m - top), axis=0, keepdims=True)
        st_out[r:r + 1, :] = top
        st_out[r + 1:r + 2, :] = 1.0 / total
    spread(st_out, st_res, st_sem)
    lax.fori_loop(HEAD_ROUNDS + 2, depth, head_round, 0)
    load_q(1)
    wait_tiles(st_res, st_sem.at[3])

    for mb in range(2):
        for h in range(halves):
            d = mb * depth * halves + h
            lanes = slice(h * LANES, (h + 1) * LANES)
            f = jnp.exp(loc_max[rounds + mb][:, lanes] - st_res[d, 2:3, :]) * st_res[d, 3:4, :]
            eb[mb, :, lanes] = eb[mb, :, lanes] * f

    def process(g, late=False):
        def wait(width):
            block = recv.at[g, pl.ds(0, (n - 1) * SUBLANES), pl.ds(0, width)]
            pltpu.make_async_copy(block, block, recv_sem.at[g]).wait()

        narrow(g, wait)
        i = lax.rem(g, depth)
        scales, picks, sums = [], [], []
        for h in range(halves):
            lanes = slice(h * LANES, (h + 1) * LANES)
            d = g * halves + h
            scales.append(jnp.exp(loc_max[g][:, lanes] - st_res[d, 0:1, :]) * st_res[d, 1:2, :])
            picks.append(tok_buf[g][:, lanes] - me * vocab)
            sums += [jnp.zeros((SUBLANES, LANES), jnp.float32)] * 3

        def tile(v, size, sums, last=False):
            line = lax.broadcasted_iota(jnp.int32, (size, LANES), 0)
            after = []
            for h in range(halves):
                lanes = slice(h * LANES, (h + 1) * LANES)
                qt = recv[g, lanes, pl.ds(v, LANES)].T
                if last:
                    guests[pl.ds(pl.multiple_of(i * gap, SUBLANES), gap), lanes] = qt[size:]
                    qt = jnp.where(i == spread_pos, guests[0:size, lanes], qt[:size])
                p = ex[g, pl.ds(v, size), lanes] * scales[h]
                x = jnp.maximum(p - qt, 0.0)
                ex[g, pl.ds(v, size), lanes] = x
                hit = line == picks[h] - v
                for k, part in enumerate((x, jnp.where(hit, qt, 0.0), jnp.where(hit, p, 0.0))):
                    fold = jnp.sum(part.reshape(size // SUBLANES, SUBLANES, LANES), axis=0)
                    after.append(sums[3 * h + k] + fold)
            return tuple(after)

        sums = lax.fori_loop(
            0, tiles - 1, lambda t, s: tile(pl.multiple_of(t * LANES, LANES), LANES, s), tuple(sums), unroll=UNROLL)
        sums = tile((tiles - 1) * LANES, used, sums, last=True)
        for h in range(halves):
            d = g * halves + h
            total, q_pick, p_pick = (jnp.sum(a, axis=0, keepdims=True) for a in sums[3 * h:3 * h + 3])
            found = (picks[h] >= 0) & (picks[h] < vocab)
            accept = jnp.where(found, jnp.minimum(p_pick / q_pick, 1.0), 0.0)
            if late:
                late_send[2 * (d - early)] = total
                late_send[2 * (d - early) + 1] = accept
                continue
            z_send[d, 0:1, :] = total
            z_send[d, 1:2, :] = accept

            @pl.when(me != d)
            def _():
                pltpu.make_async_remote_copy(
                    src_ref=z_send.at[d], dst_ref=z_recv.at[me], send_sem=z_sem.at[0], recv_sem=z_sem.at[1],
                    device_id={'tp': d}, device_id_type=MESH).start()

            @pl.when(me == d)
            def _():
                z_recv[me] = z_send[d]

    wait_q()

    def main_round(r, carry):
        wait_send(r - SLOTS)
        pack(r)
        send(r)
        process(r - SLOTS)
        return carry

    lax.fori_loop(depth, rounds, main_round, 0)

    def tail_round(g, carry):
        process(g)
        return carry

    lax.fori_loop(rounds - SLOTS, rounds - LATE_ROUNDS, tail_round, 0)
    for g in range(rounds - LATE_ROUNDS, rounds - 1):
        process(g, late=True)

    @pl.when(me < early)
    def _():
        wait_tiles(z_recv, z_sem.at[1])
        sums = jnp.sum(z_recv[...], axis=0)
        z_out[0:1, :] = 1.0 / sums[0:1]
        z_out[1:2, :] = sums[1:2]
        spread(z_out, z_res, z_sem)

    process(rounds - 1, late=True)
    spread(late_send, late_recv, late_sem)

    def drain(r, carry):
        wait_send(r)
        return carry

    lax.fori_loop(rounds - SLOTS, rounds, drain, 0)
    wait_tiles(st_send, st_sem.at[0])
    wait_tiles(st_res, st_sem.at[2])

    def wait_some(ref, count, sem):
        block = ref.at[pl.ds(0, count)]
        pltpu.make_async_copy(block, block, sem).wait()

    @pl.when(me < early)
    def _():
        wait_some(z_send, early - 1, z_sem.at[0])
        wait_tiles(z_res, z_sem.at[2])
        wait_some(z_res, early - 1, z_sem.at[3])

    @pl.when(me >= early)
    def _():
        wait_some(z_send, early, z_sem.at[0])
        wait_some(z_res, early, z_sem.at[3])

    fin[0:early] = z_res[0:early]
    wait_tiles(late_recv, late_sem.at[3])
    late = jnp.sum(late_recv[...], axis=0)
    for k in range(n - early):
        fin[early + k, 0:1, :] = 1.0 / late[2 * k]
        fin[early + k, 1:2, :] = late[2 * k + 1]
    wait_tiles(late_recv, late_sem.at[2])


def finish_kernel(depth, ex, eb, fin, res_one, res_two, bon_one, bon_two, acc_one, acc_two, exp_one, exp_two,
                  buf, sem, b_sem):
    ress, bons, accs, exps = (res_one, res_two), (bon_one, bon_two), (acc_one, acc_two), (exp_one, exp_two)
    halves = eb.shape[2] // LANES
    slots = buf.shape[0]
    for mb in range(2):
        pltpu.make_async_copy(eb.at[mb], bons[mb], b_sem.at[mb]).start()
    pending = []
    for mb in range(2):
        for i in range(depth):
            g = mb * depth + i
            if g >= slots:
                pending[g - slots].wait()
            for h in range(halves):
                lanes = slice(h * LANES, (h + 1) * LANES)
                buf[g % slots, :, lanes] = ex[g, :, lanes] * fin[g * halves + h, 0:1, :]
            copy = pltpu.make_async_copy(buf.at[g % slots], ress[mb].at[i], sem.at[g % slots])
            copy.start()
            pending.append(copy)
    for mb in range(2):
        for h in range(halves):
            lanes = slice(h * LANES, (h + 1) * LANES)
            prod = jnp.ones((1, LANES), jnp.float32)
            total = jnp.zeros((1, LANES), jnp.float32)
            for i in range(depth):
                a = fin[(mb * depth + i) * halves + h, 1:2, :]
                accs[mb][i:i + 1, lanes] = a
                prod = prod * a
                total = total + prod
            exps[mb][:, lanes] = total
    for copy in pending[-slots:]:
        copy.wait()
    for mb in range(2):
        pltpu.make_async_copy(eb.at[mb], bons[mb], b_sem.at[mb]).wait()


def verify_both(n, hid_one, q_one, tok_one, hid_two, q_two, tok_two, w_local):
    seqs, depth, whole_vocab = q_one.shape
    batch, vocab, hidden = hid_one.shape[0], w_local.shape[1], hid_one.shape[2]
    halves = batch // LANES
    rounds = 2 * depth
    width = pl.cdiv(vocab, LANES) * LANES
    assert seqs == SUBLANES and rounds * halves == n and batch == n * seqs
    f32 = jnp.float32
    vmem = pl.BlockSpec(memory_space=pltpu.VMEM)
    anys = pl.BlockSpec(memory_space=pl.ANY)
    late = (2 * LATE_ROUNDS * halves, 1, LANES)
    ex, eb, fin = pl.pallas_call(
        functools.partial(exchange_kernel, n),
        out_shape=(pltpu.VMEM((rounds, vocab, batch), f32), pltpu.VMEM((2, vocab, batch), f32), pltpu.VMEM((n, 2, LANES), f32)),
        in_specs=[anys, anys, anys, anys, vmem, vmem, anys],
        out_specs=(vmem, vmem, vmem),
        scratch_shapes=[
            pltpu.VMEM((vocab, hidden), w_local.dtype),
            pltpu.VMEM((2, batch, hidden), hid_one.dtype),
            pltpu.VMEM((whole_vocab // LANES + 1, seqs * depth, LANES), f32),
            pltpu.VMEM((SLOTS, n, SUBLANES, width), f32),
            pltpu.VMEM((rounds, batch, width), f32),
            pltpu.VMEM((rounds + 2, 1, batch), f32),
            pltpu.VMEM((rounds, 1, batch), jnp.int32),
            pltpu.VMEM((n, 4, LANES), f32), pltpu.VMEM((n, 4, LANES), f32), pltpu.VMEM((4, LANES), f32), pltpu.VMEM((n, 4, LANES), f32),
            pltpu.VMEM((n, 2, LANES), f32), pltpu.VMEM((n, 2, LANES), f32), pltpu.VMEM((2, LANES), f32), pltpu.VMEM((n, 2, LANES), f32),
            pltpu.VMEM(late, f32), pltpu.VMEM((n,) + late, f32), pltpu.VMEM((depth * (width - vocab), batch), f32),
            pltpu.SemaphoreType.DMA, pltpu.SemaphoreType.DMA, pltpu.SemaphoreType.DMA((2,)),
            pltpu.SemaphoreType.DMA((SLOTS,)), pltpu.SemaphoreType.DMA((rounds,)),
            pltpu.SemaphoreType.DMA((4,)), pltpu.SemaphoreType.DMA((4,)), pltpu.SemaphoreType.DMA((4,)),
        ],
        compiler_params=pltpu.CompilerParams(collective_id=0, has_side_effects=True, vmem_limit_bytes=44 * 2 ** 20),
        name='exchange',
    )(jnp.swapaxes(hid_one, 0, 1), jnp.swapaxes(hid_two, 0, 1),
      q_one.reshape(seqs * depth, whole_vocab), q_two.reshape(seqs * depth, whole_vocab),
      tok_one.T, tok_two.T, w_local.T)

    shapes = [(depth, vocab, batch)] * 2 + [(vocab, batch)] * 2 + [(depth, batch)] * 2 + [(1, batch)] * 2
    outs = pl.pallas_call(
        functools.partial(finish_kernel, depth),
        out_shape=[jax.ShapeDtypeStruct(s, f32) for s in shapes],
        in_specs=[vmem] * 3,
        out_specs=[anys] * 4 + [vmem] * 4,
        scratch_shapes=[pltpu.VMEM((4, vocab, batch), f32), pltpu.SemaphoreType.DMA((4,)), pltpu.SemaphoreType.DMA((2,))],
        compiler_params=pltpu.CompilerParams(vmem_limit_bytes=12 * 2 ** 20),
        name='finish',
    )(ex, eb, fin)
    res, bon, acc, tot = outs[0:2], outs[2:4], outs[4:6], outs[6:8]
    result = ()
    for mb in range(2):
        result += (acc[mb].T, tot[mb].reshape(batch), jnp.transpose(res[mb], (2, 0, 1)), bon[mb].T)
    return result


def solution(mesh):
    row_spec = P('dp')
    q_spec = P(('dp', 'tp'))
    w_spec = P(None, 'tp')
    vocab_spec = P('dp', None, 'tp')
    bonus_spec = P('dp', 'tp')
    out_specs = (row_spec, row_spec, vocab_spec, bonus_spec) * 2
    in_specs = (row_spec, q_spec, row_spec, row_spec, q_spec, row_spec, w_spec)
    return jax.shard_map(functools.partial(verify_both, mesh.shape['tp']), mesh=mesh,
                         in_specs=in_specs, out_specs=out_specs, check_vma=False)
```

```python
import functools
import math

import jax
import jax.numpy as jnp
from jax import lax
from jax.experimental import pallas as pl
from jax.experimental.pallas import tpu as pltpu
from jax.sharding import PartitionSpec as P

INV_TEMP = 1.25
LANES = 128
SUBLANES = 8
SLOTS = 8
HEAD_ROUNDS = 4
COL_TILE = 256
LATE_ROUNDS = 2
UNROLL = 7
PACK_UNROLL = 4
CHUNKS = 4
MESH = pl.DeviceIdType.MESH


def partner_steps(side):
    one, back, half = 1, side - 1, side // 2
    classes = [
        [(half, one), (half, back), (one, half), (back, half)],
        [(half, half)],
        [(half, 0), (0, half)],
        [(one, one), (back, back)],
        [(one, back), (back, one)],
        [(one, 0), (back, 0), (0, one), (0, back)],
        [(0, 0)],
    ]
    assert sorted(d for c in classes for d in c) == [(x, y) for x in range(side) for y in range(side)]
    return [(dx, dy, dc) for c in classes for dc in range(2) for dx, dy in c if (dx, dy, dc) != (0, 0, 0)]


def exchange_kernel(n, hid_one, hid_two, q_one, q_two, tok_one, tok_two, w_hbm,
                    ex, eb, fin,
                    w_buf, hid_buf, q_buf, stage, recv, loc_max, tok_buf,
                    st_send, st_recv, st_out, st_res, z_send, z_recv, z_out, z_res, late_send, late_recv, guests,
                    q_sem, w_sem, hid_sem, send_sem, recv_sem, st_sem, z_sem, late_sem):
    me = lax.axis_index('tp')
    depth, batch = tok_one.shape
    vocab = w_hbm.shape[0]
    halves = batch // LANES
    rounds = 2 * depth
    early = (rounds - LATE_ROUNDS) * halves
    hids, qs, toks = (hid_one, hid_two), (q_one, q_two), (tok_one, tok_two)
    side = math.isqrt(n // 2)
    core, chip = lax.rem(me, 2), me // 2
    col, row = lax.rem(chip, side), chip // side
    steps = partner_steps(side)

    def partner(step):
        dx, dy, dc = step
        dy = dy + core * ((side - dy) % side - dy)
        return (lax.rem(row + dy, side) * side + lax.rem(col + dx, side)) * 2 + lax.rem(core + dc, 2)

    barrier = pltpu.get_barrier_semaphore()
    for step in steps:
        pl.semaphore_signal(barrier, inc=1, device_id={'tp': partner(step)}, device_id_type=MESH)

    seqs, q_tiles = q_one.shape[0], q_one.shape[1] // depth
    pitch = (q_tiles + 1) * depth
    tiles = pl.cdiv(vocab, LANES)
    share = n // CHUNKS
    ends = [min(q_tiles, ((k + 1) * share - 1) * vocab // LANES + tiles + 1) for k in range(CHUNKS)]
    chunks = list(zip([0] + ends[:-1], ends))

    def load_q(mb):
        for k, (low, high) in enumerate(chunks):
            for b in range(seqs):
                pltpu.make_async_copy(
                    qs[mb].at[b, pl.ds(low * depth, (high - low) * depth)],
                    q_buf.at[pl.ds(b * pitch + low * depth, (high - low) * depth)], q_sem.at[k]).start()

    def wait_q(k):
        low, high = chunks[k]
        block = q_buf.at[pl.ds(0, seqs * (high - low) * depth)]
        pltpu.make_async_copy(block, block, q_sem.at[k]).wait()

    def load_hid(mb, i, slot):
        return pltpu.make_async_copy(hids[mb].at[i], hid_buf.at[slot], hid_sem.at[slot])

    load_q(0)
    load_w = pltpu.make_async_copy(w_hbm, w_buf, w_sem)
    load_w.start()
    load_hid(0, 0, 0).start()
    for g in range(rounds):
        i = g % depth
        tok_buf[g] = toks[g // depth][i:i + 1, :]
    lane = lax.broadcasted_iota(jnp.int32, (SUBLANES, LANES), 1)
    used = vocab - (tiles - 1) * LANES
    gap = LANES - used
    spread_pos = pl.cdiv(used, gap)
    assert spread_pos < depth and gap % SUBLANES == 0

    def narrow(r, action):
        @pl.when(lax.rem(r, depth) == spread_pos)
        def _():
            action((tiles - 1) * LANES)

        @pl.when(lax.rem(r, depth) != spread_pos)
        def _():
            action(tiles * LANES)

    def pack(r, first=0, count=n):
        i, slot = lax.rem(r, depth), lax.rem(r, SLOTS)
        to_gap = lax.rem(used + depth * LANES - gap * i, LANES)

        def one(d, carry):
            start = d * vocab
            base, off = start // LANES, lax.rem(start, LANES)
            shift = lax.rem(LANES - off, LANES)
            rolled = []
            for t in range(tiles + 1):
                rolled.append(pltpu.roll(q_buf[pl.ds((base + t) * depth + i, seqs, stride=pitch), :], shift, 1))
            for t in range(tiles - 1):
                stage[slot, d, :, t * LANES:(t + 1) * LANES] = jnp.where(lane < LANES - off, rolled[t], rolled[t + 1])
            last = jnp.where(lane < LANES - off, rolled[tiles - 1], rolled[tiles])
            guest = [pltpu.roll(q_buf[pl.ds((base + t) * depth + spread_pos, seqs, stride=pitch), :], shift, 1)
                     for t in (tiles - 1, tiles)]
            guest = pltpu.roll(jnp.where(lane < LANES - off, guest[0], guest[1]), to_gap, 1)
            stage[slot, d, :, (tiles - 1) * LANES:] = jnp.where(lane < used, last, guest)
            return carry

        lax.fori_loop(first, first + count, one, 0, unroll=PACK_UNROLL)

    def send(r):
        slot = lax.rem(r, SLOTS)
        mine = pl.ds(pl.multiple_of(me * SUBLANES, SUBLANES), SUBLANES)

        def start(width):
            for step in steps:
                to = partner(step)
                pltpu.make_async_remote_copy(
                    src_ref=stage.at[slot, to, :, pl.ds(0, width)], dst_ref=recv.at[r, mine, pl.ds(0, width)],
                    send_sem=send_sem.at[slot], recv_sem=recv_sem.at[r],
                    device_id={'tp': to}, device_id_type=MESH).start()

        narrow(r, start)
        recv[r, mine, :] = stage[slot, me]

    def wait_send(r):
        def wait(width):
            block = stage.at[lax.rem(r, SLOTS), pl.ds(0, n - 1), :, pl.ds(0, width)]
            pltpu.make_async_copy(block, block, send_sem.at[lax.rem(r, SLOTS)]).wait()

        narrow(r, wait)

    def wait_tiles(ref, sem):
        block = ref.at[pl.ds(0, n - 1)]
        pltpu.make_async_copy(block, block, sem).wait()

    for k in range(CHUNKS):
        wait_q(k)
        pack(0, k * share, share)
    pl.semaphore_wait(barrier, n - 1)
    send(0)

    def head_round(r, carry):
        pack(r)
        send(r)
        return carry

    lax.fori_loop(1, HEAD_ROUNDS, head_round, 0)

    load_w.wait()
    spans = [(v, min(COL_TILE, vocab - v)) for v in range(0, vocab, COL_TILE)]

    def logits(hid_slot, out):
        top = None
        for v, size in spans:
            z = lax.dot_general(w_buf[v:v + size, :], hid_buf[hid_slot], (((1,), (1,)), ((), ())),
                                preferred_element_type=jnp.float32) * INV_TEMP
            out[v:v + size, :] = z
            m = jnp.max(z, axis=0, keepdims=True)
            top = m if top is None else jnp.maximum(top, m)
        total = jnp.zeros_like(top)
        for v, size in spans:
            e = jnp.exp(out[v:v + size, :] - top)
            out[v:v + size, :] = e
            total = total + jnp.sum(e, axis=0, keepdims=True)
        return top, total

    for mb in range(2):
        first = mb * (depth + 1)

        def position(i, carry, mb=mb, first=first):
            slot = lax.rem(first + i, 2)
            load_hid(mb, i + 1, 1 - slot).start()
            load_hid(mb, i, slot).wait()
            g = mb * depth + i
            top, total = logits(slot, ex.at[g])
            loc_max[g] = top
            for h in range(halves):
                st_send[g * halves + h, 0:1, :] = top[:, h * LANES:(h + 1) * LANES]
                st_send[g * halves + h, 1:2, :] = total[:, h * LANES:(h + 1) * LANES]
            return carry

        lax.fori_loop(0, depth, position, 0)
        slot = (first + depth) % 2
        if mb == 0:
            load_hid(1, 0, 1 - slot).start()
        load_hid(mb, depth, slot).wait()
        top, total = logits(slot, eb.at[mb])
        loc_max[rounds + mb] = top
        for i in range(depth):
            for h in range(halves):
                d = (mb * depth + i) * halves + h
                st_send[d, 2:3, :] = top[:, h * LANES:(h + 1) * LANES]
                st_send[d, 3:4, :] = total[:, h * LANES:(h + 1) * LANES]

    def scatter(src, dst, sems):
        for step in steps:
            to = partner(step)
            pltpu.make_async_remote_copy(
                src_ref=src.at[to], dst_ref=dst.at[me], send_sem=sems.at[0], recv_sem=sems.at[1],
                device_id={'tp': to}, device_id_type=MESH).start()
        dst[me] = src[me]

    def spread(src, dst, sems):
        for step in steps:
            pltpu.make_async_remote_copy(
                src_ref=src, dst_ref=dst.at[me], send_sem=sems.at[2], recv_sem=sems.at[3],
                device_id={'tp': partner(step)}, device_id_type=MESH).start()
        dst[me] = src[...]

    scatter(st_send, st_recv, st_sem)
    lax.fori_loop(HEAD_ROUNDS, HEAD_ROUNDS + 2, head_round, 0)
    wait_tiles(st_recv, st_sem.at[1])
    for r in (0, 2):
        m = st_recv[:, r, :]
        top = jnp.max(m, axis=0, keepdims=True)
        total = jnp.sum(st_recv[:, r + 1, :] * jnp.exp(m - top), axis=0, keepdims=True)
        st_out[r:r + 1, :] = top
        st_out[r + 1:r + 2, :] = 1.0 / total
    spread(st_out, st_res, st_sem)
    lax.fori_loop(HEAD_ROUNDS + 2, depth, head_round, 0)
    load_q(1)
    wait_tiles(st_res, st_sem.at[3])

    for mb in range(2):
        for h in range(halves):
            d = mb * depth * halves + h
            lanes = slice(h * LANES, (h + 1) * LANES)
            f = jnp.exp(loc_max[rounds + mb][:, lanes] - st_res[d, 2:3, :]) * st_res[d, 3:4, :]
            eb[mb, :, lanes] = eb[mb, :, lanes] * f

    def process(g, late=False):
        def wait(width):
            block = recv.at[g, pl.ds(0, (n - 1) * SUBLANES), pl.ds(0, width)]
            pltpu.make_async_copy(block, block, recv_sem.at[g]).wait()

        narrow(g, wait)
        i = lax.rem(g, depth)
        scales, picks, sums = [], [], []
        for h in range(halves):
            lanes = slice(h * LANES, (h + 1) * LANES)
            d = g * halves + h
            scales.append(jnp.exp(loc_max[g][:, lanes] - st_res[d, 0:1, :]) * st_res[d, 1:2, :])
            picks.append(tok_buf[g][:, lanes] - me * vocab)
            sums += [jnp.zeros((SUBLANES, LANES), jnp.float32)] * 3

        def tile(v, size, sums, last=False):
            line = lax.broadcasted_iota(jnp.int32, (size, LANES), 0)
            after = []
            for h in range(halves):
                lanes = slice(h * LANES, (h + 1) * LANES)
                qt = recv[g, lanes, pl.ds(v, LANES)].T
                if last:
                    guests[pl.ds(pl.multiple_of(i * gap, SUBLANES), gap), lanes] = qt[size:]
                    qt = jnp.where(i == spread_pos, guests[0:size, lanes], qt[:size])
                p = ex[g, pl.ds(v, size), lanes] * scales[h]
                x = jnp.maximum(p - qt, 0.0)
                ex[g, pl.ds(v, size), lanes] = x
                hit = line == picks[h] - v
                for k, part in enumerate((x, jnp.where(hit, qt, 0.0), jnp.where(hit, p, 0.0))):
                    fold = jnp.sum(part.reshape(size // SUBLANES, SUBLANES, LANES), axis=0)
                    after.append(sums[3 * h + k] + fold)
            return tuple(after)

        sums = lax.fori_loop(
            0, tiles - 1, lambda t, s: tile(pl.multiple_of(t * LANES, LANES), LANES, s), tuple(sums), unroll=UNROLL)
        sums = tile((tiles - 1) * LANES, used, sums, last=True)
        for h in range(halves):
            d = g * halves + h
            total, q_pick, p_pick = (jnp.sum(a, axis=0, keepdims=True) for a in sums[3 * h:3 * h + 3])
            found = (picks[h] >= 0) & (picks[h] < vocab)
            accept = jnp.where(found, jnp.minimum(p_pick / q_pick, 1.0), 0.0)
            if late:
                late_send[2 * (d - early)] = total
                late_send[2 * (d - early) + 1] = accept
                continue
            z_send[d, 0:1, :] = total
            z_send[d, 1:2, :] = accept

            @pl.when(me != d)
            def _():
                pltpu.make_async_remote_copy(
                    src_ref=z_send.at[d], dst_ref=z_recv.at[me], send_sem=z_sem.at[0], recv_sem=z_sem.at[1],
                    device_id={'tp': d}, device_id_type=MESH).start()

            @pl.when(me == d)
            def _():
                z_recv[me] = z_send[d]

    for k in range(CHUNKS):
        wait_q(k)

    def main_round(r, carry):
        wait_send(r - SLOTS)
        pack(r)
        send(r)
        process(r - SLOTS)
        return carry

    lax.fori_loop(depth, rounds, main_round, 0)

    def tail_round(g, carry):
        process(g)
        return carry

    lax.fori_loop(rounds - SLOTS, rounds - LATE_ROUNDS, tail_round, 0)
    for g in range(rounds - LATE_ROUNDS, rounds - 1):
        process(g, late=True)

    @pl.when(me < early)
    def _():
        wait_tiles(z_recv, z_sem.at[1])
        sums = jnp.sum(z_recv[...], axis=0)
        z_out[0:1, :] = 1.0 / sums[0:1]
        z_out[1:2, :] = sums[1:2]
        spread(z_out, z_res, z_sem)

    process(rounds - 1, late=True)
    spread(late_send, late_recv, late_sem)

    def drain(r, carry):
        wait_send(r)
        return carry

    lax.fori_loop(rounds - SLOTS, rounds, drain, 0)
    wait_tiles(st_send, st_sem.at[0])
    wait_tiles(st_res, st_sem.at[2])

    def wait_some(ref, count, sem):
        block = ref.at[pl.ds(0, count)]
        pltpu.make_async_copy(block, block, sem).wait()

    @pl.when(me < early)
    def _():
        wait_some(z_send, early - 1, z_sem.at[0])
        wait_tiles(z_res, z_sem.at[2])
        wait_some(z_res, early - 1, z_sem.at[3])

    @pl.when(me >= early)
    def _():
        wait_some(z_send, early, z_sem.at[0])
        wait_some(z_res, early, z_sem.at[3])

    fin[0:early] = z_res[0:early]
    wait_tiles(late_recv, late_sem.at[3])
    late = jnp.sum(late_recv[...], axis=0)
    for k in range(n - early):
        fin[early + k, 0:1, :] = 1.0 / late[2 * k]
        fin[early + k, 1:2, :] = late[2 * k + 1]
    wait_tiles(late_recv, late_sem.at[2])


def finish_kernel(depth, ex, eb, fin, res_one, res_two, bon_one, bon_two, acc_one, acc_two, exp_one, exp_two,
                  buf, sem, b_sem):
    ress, bons, accs, exps = (res_one, res_two), (bon_one, bon_two), (acc_one, acc_two), (exp_one, exp_two)
    halves = eb.shape[2] // LANES
    slots = buf.shape[0]
    for mb in range(2):
        pltpu.make_async_copy(eb.at[mb], bons[mb], b_sem.at[mb]).start()
    pending = []
    for mb in range(2):
        for i in range(depth):
            g = mb * depth + i
            if g >= slots:
                pending[g - slots].wait()
            for h in range(halves):
                lanes = slice(h * LANES, (h + 1) * LANES)
                buf[g % slots, :, lanes] = ex[g, :, lanes] * fin[g * halves + h, 0:1, :]
            copy = pltpu.make_async_copy(buf.at[g % slots], ress[mb].at[i], sem.at[g % slots])
            copy.start()
            pending.append(copy)
    for mb in range(2):
        for h in range(halves):
            lanes = slice(h * LANES, (h + 1) * LANES)
            prod = jnp.ones((1, LANES), jnp.float32)
            total = jnp.zeros((1, LANES), jnp.float32)
            for i in range(depth):
                a = fin[(mb * depth + i) * halves + h, 1:2, :]
                accs[mb][i:i + 1, lanes] = a
                prod = prod * a
                total = total + prod
            exps[mb][:, lanes] = total
    for copy in pending[-slots:]:
        copy.wait()
    for mb in range(2):
        pltpu.make_async_copy(eb.at[mb], bons[mb], b_sem.at[mb]).wait()


def verify_both(n, hid_one, q_one, tok_one, hid_two, q_two, tok_two, w_local):
    seqs, depth, whole_vocab = q_one.shape
    batch, vocab, hidden = hid_one.shape[0], w_local.shape[1], hid_one.shape[2]
    halves = batch // LANES
    rounds = 2 * depth
    width = pl.cdiv(vocab, LANES) * LANES
    assert seqs == SUBLANES and depth == SUBLANES and rounds * halves == n and batch == n * seqs
    f32 = jnp.float32
    vmem = pl.BlockSpec(memory_space=pltpu.VMEM)
    anys = pl.BlockSpec(memory_space=pl.ANY)
    late = (2 * LATE_ROUNDS * halves, 1, LANES)

    def by_tile(q):
        q = q.reshape(seqs, depth, whole_vocab // LANES, LANES)
        return jnp.swapaxes(q, 1, 2).reshape(seqs, whole_vocab // LANES * depth, LANES)

    ex, eb, fin = pl.pallas_call(
        functools.partial(exchange_kernel, n),
        out_shape=(pltpu.VMEM((rounds, vocab, batch), f32), pltpu.VMEM((2, vocab, batch), f32), pltpu.VMEM((n, 2, LANES), f32)),
        in_specs=[anys, anys, anys, anys, vmem, vmem, anys],
        out_specs=(vmem, vmem, vmem),
        scratch_shapes=[
            pltpu.VMEM((vocab, hidden), w_local.dtype),
            pltpu.VMEM((2, batch, hidden), hid_one.dtype),
            pltpu.VMEM((seqs * (whole_vocab // LANES + 1) * depth, LANES), f32),
            pltpu.VMEM((SLOTS, n, SUBLANES, width), f32),
            pltpu.VMEM((rounds, batch, width), f32),
            pltpu.VMEM((rounds + 2, 1, batch), f32),
            pltpu.VMEM((rounds, 1, batch), jnp.int32),
            pltpu.VMEM((n, 4, LANES), f32), pltpu.VMEM((n, 4, LANES), f32), pltpu.VMEM((4, LANES), f32), pltpu.VMEM((n, 4, LANES), f32),
            pltpu.VMEM((n, 2, LANES), f32), pltpu.VMEM((n, 2, LANES), f32), pltpu.VMEM((2, LANES), f32), pltpu.VMEM((n, 2, LANES), f32),
            pltpu.VMEM(late, f32), pltpu.VMEM((n,) + late, f32), pltpu.VMEM((depth * (width - vocab), batch), f32),
            pltpu.SemaphoreType.DMA((CHUNKS,)), pltpu.SemaphoreType.DMA, pltpu.SemaphoreType.DMA((2,)),
            pltpu.SemaphoreType.DMA((SLOTS,)), pltpu.SemaphoreType.DMA((rounds,)),
            pltpu.SemaphoreType.DMA((4,)), pltpu.SemaphoreType.DMA((4,)), pltpu.SemaphoreType.DMA((4,)),
        ],
        compiler_params=pltpu.CompilerParams(collective_id=0, has_side_effects=True, vmem_limit_bytes=44 * 2 ** 20),
        name='exchange',
    )(jnp.swapaxes(hid_one, 0, 1), jnp.swapaxes(hid_two, 0, 1),
      by_tile(q_one), by_tile(q_two),
      tok_one.T, tok_two.T, w_local.T)

    shapes = [(depth, vocab, batch)] * 2 + [(vocab, batch)] * 2 + [(depth, batch)] * 2 + [(1, batch)] * 2
    outs = pl.pallas_call(
        functools.partial(finish_kernel, depth),
        out_shape=[jax.ShapeDtypeStruct(s, f32) for s in shapes],
        in_specs=[vmem] * 3,
        out_specs=[anys] * 4 + [vmem] * 4,
        scratch_shapes=[pltpu.VMEM((4, vocab, batch), f32), pltpu.SemaphoreType.DMA((4,)), pltpu.SemaphoreType.DMA((2,))],
        compiler_params=pltpu.CompilerParams(vmem_limit_bytes=12 * 2 ** 20),
        name='finish',
    )(ex, eb, fin)
    res, bon, acc, tot = outs[0:2], outs[2:4], outs[4:6], outs[6:8]
    result = ()
    for mb in range(2):
        result += (acc[mb].T, tot[mb].reshape(batch), jnp.transpose(res[mb], (2, 0, 1)), bon[mb].T)
    return result


def solution(mesh):
    row_spec = P('dp')
    q_spec = P(('dp', 'tp'))
    w_spec = P(None, 'tp')
    vocab_spec = P('dp', None, 'tp')
    bonus_spec = P('dp', 'tp')
    out_specs = (row_spec, row_spec, vocab_spec, bonus_spec) * 2
    in_specs = (row_spec, q_spec, row_spec, row_spec, q_spec, row_spec, w_spec)
    return jax.shard_map(functools.partial(verify_both, mesh.shape['tp']), mesh=mesh,
                         in_specs=in_specs, out_specs=out_specs, check_vma=False)
```
